256 devices in a mesh: row: 8 (over y, x_lo), col: 16 (over z, core), layer: 2 (over x_hi).
Axes of the slice: x: 4 (x_hi: 2, x_lo: 2; x = x_hi * 2 + x_lo), y: 4, z: 8, core: 2. Of those that a mesh axis runs over, the one named last changes fastest.
Arguments:
- tokens: bfloat16 [10240, 8192], P('row', 'col'), may hold values from -6 to 6
- up_weight: bfloat16 [8192, 16384], P('row', 'col'), may hold values from -0.0625 to 0.0625
Outputs:
- up: bfloat16 [10240, 16384], P('row', ('col', 'layer'))
The draws below stay inside these ranges and needn't reach their ends.
All inputs are finite; a program needn't handle non-finite values.
Results may differ from the reference program's by a relative error of at most 0.001.
Values may be sent and summed in bfloat16 or wider, within the bound.
No kernel may reach another device: no remote copies, remote signals or barrier semaphores. Data moves between devices by JAX's collectives and lax.ppermute only.
A program may use at most 128 MiB of HBM per device.

```python
import jax
import jax.numpy as jnp

D = 8192
FFN = 16384
TOKENS = 10240


def block_levels(rng, dims, shards, smallest, high):
    def one(axis_at, parts):
        steps = jax.random.uniform(jax.random.fold_in(jax.random.fold_in(rng, 6), axis_at), (parts,), jnp.float32, smallest / len(shards), high / len(shards))
        return jnp.repeat(jnp.exp(steps), dims[axis_at] // parts).reshape((-1,) + (1,) * (len(dims) - axis_at - 1))

    factor_of = one(*shards[0])
    for cut in shards[1:]:
        factor_of = factor_of * one(*cut)
    return factor_of


def noise(stream_key, extent, scale, reach, shards=(), dtype=jnp.bfloat16):
    array = scale * jax.random.normal(stream_key, extent, jnp.float32)
    if shards:
        array = array * block_levels(stream_key, extent, shards, -0.22, 0.18)
    return jnp.clip(array, -reach, reach).astype(dtype)


def setup_inputs(seed: int = 0) -> dict:
    key_list = jax.random.split(jax.random.key(seed), 3)
    tokens = noise(key_list[0], (TOKENS, D), 1.0, 6.0, ((0, 8), (1, 16)))
    up_weight = noise(key_list[1], (D, FFN), D ** -0.5, 0.0625, ((0, 8), (1, 16)))
    return dict(tokens=tokens, up_weight=up_weight)


def reference(tokens, up_weight):
    product = jnp.dot(tokens, up_weight, preferred_element_type=jnp.float32)
    return product.astype(jnp.bfloat16)
```

```python
import jax
import jax.numpy as jnp
from jax import lax
from jax.sharding import Mesh
from jax.sharding import PartitionSpec as P


AXES = ("y", "xl", "z", "core", "xh")


def ring(size, shift):
    return [(i, (i + shift) % size) for i in range(size)]


def per_device(tokens, up_weight):
    y, xl, z, core, xh = (lax.axis_index(name) for name in AXES)
    zn, yn = lax.axis_size("z"), lax.axis_size("y")
    rows, depth = tokens.shape
    half = rows // 2
    width = up_weight.shape[1] // 2

    def zup(a):
        return lax.ppermute(a, "z", ring(zn, 1))

    def zdown(a):
        return lax.ppermute(a, "z", ring(zn, -1))

    def yup(a):
        return lax.ppermute(a, "y", ring(yn, 1))

    def ydown(a):
        return lax.ppermute(a, "y", ring(yn, -1))

    def peer(a):
        return lax.ppermute(a, "xh", ring(2, 1))

    mine = lax.dynamic_slice_in_dim(up_weight, core * depth, depth, 0)
    given = lax.dynamic_slice_in_dim(up_weight, (1 - core) * depth, depth, 0)

    own, oth = {}, {}
    own[0] = lax.dynamic_slice_in_dim(tokens, xh * half, half, 0)
    oth[0] = lax.dynamic_slice_in_dim(tokens, (1 - xh) * half, half, 0)
    own[-1] = zup(own[0])
    own[1] = zdown(own[0])
    got = lax.ppermute(given, "core", ring(2, 1))

    def both(part, layer):
        return jnp.concatenate(
            [lax.dynamic_slice_in_dim(a, layer * width, width, 1) for a in part], 1
        )

    quarter = depth // 2
    wa, wb = {}, {}
    wa[0] = both((mine, got), xh)
    far = both((mine[quarter:], got[quarter:]), 1 - xh)
    near_got = lax.ppermute(wa[0][:quarter], "xl", ring(2, 1))
    far_got = lax.ppermute(far, ("xl", "xh"), [(2, 1), (1, 2), (3, 0), (0, 3)])
    wa[-1] = yup(wa[0])
    wa[1] = ydown(wa[0])
    wb[0] = jnp.concatenate([near_got, far_got], 0)
    wb[-1] = yup(wb[0])
    wb[1] = ydown(wb[0])
    wa[2] = yup(wa[-1])
    wb[2] = ydown(wb[1])

    own[-2] = zup(own[-1])
    own[2] = zdown(own[1])
    own[-3] = zup(own[-2])
    own[3] = zdown(own[2])
    own[-4] = zup(own[-3])
    oth[1] = peer(own[1])
    oth[-1] = peer(own[-1])
    oth[-3] = peer(own[-3])
    oth[-4] = peer(own[-4])
    oth[2] = zdown(oth[1])
    oth[3] = zdown(oth[2])
    oth[-2] = zup(oth[-1])

    def gathered(pieces, order):
        buffer = jnp.zeros((half, zn * depth), tokens.dtype)
        for d in order:
            buffer = lax.dynamic_update_slice(buffer, pieces[d], (0, (d % zn) * depth))
        return buffer

    t_own = gathered(own, (0, -1, 1, -2, 2, -3, 3, -4))
    t_oth = gathered(oth, (0, 1, -1, 2, -3, -2, 3, -4))
    weight = jnp.zeros((zn * depth, 2 * width), up_weight.dtype)
    for pieces, side in ((wa, xl), (wb, 1 - xl)):
        for dy in (0, -1, 1, 2):
            block = 2 * ((y + dy) % yn) + side
            at = ((block - z) % zn) * depth
            weight = lax.dynamic_update_slice(weight, pieces[dy], (at, 0))
    w_own, w_partner = weight[:, :width], weight[:, width:]

    def dot(a, b):
        return jnp.dot(a, b, preferred_element_type=jnp.float32)

    sent_own = lax.ppermute(dot(t_own, w_partner), "core", ring(2, 1))
    sent_oth = lax.ppermute(dot(t_oth, w_partner), "core", ring(2, 1))
    r_own = (dot(t_own, w_own) + sent_own).astype(jnp.bfloat16)
    r_oth = (dot(t_oth, w_own) + sent_oth).astype(jnp.bfloat16)
    first = jnp.where(xh == 0, r_own, r_oth)
    second = jnp.where(xh == 0, r_oth, r_own)
    return jnp.concatenate([first, second], 0)


def solution(mesh):
    split = Mesh(
        mesh.devices.reshape(4, 2, mesh.shape["col"] // 2, 2, mesh.shape["layer"]), AXES
    )
    spec = P(("y", "xl"), ("z", "core"))
    return jax.shard_map(
        per_device,
        mesh=split,
        in_specs=(spec, spec),
        out_specs=P(("y", "xl"), ("z", "core", "xh")),
        check_vma=False,
    )
```

```python
import jax
import jax.numpy as jnp
from jax import lax
from jax.experimental import pallas as pl
from jax.experimental.pallas import tpu as pltpu
from jax.sharding import Mesh
from jax.sharding import PartitionSpec as P


AXES = ("y", "xl", "z", "core", "xh")
ROWS = 256


def ring(size, shift):
    return [(i, (i + shift) % size) for i in range(size)]


def product_kernel(counts, *refs):
    zn, yn, na, nb = counts
    a_refs, b_refs, c_refs = refs[:zn], refs[zn : 2 * zn], refs[2 * zn : 3 * zn]
    w_refs = refs[3 * zn : 4 * zn]
    out_ref, t_buf, w_buf, acc, sem, out_sem = refs[4 * zn :]
    y, xl, z, xh = (lax.axis_index(name) for name in ("y", "xl", "z", "xh"))
    width = w_buf.shape[2]

    def token_copies(d, slot):
        at = pl.multiple_of(xh * nb, nb)
        other = pl.multiple_of((1 - xh) * nb, nb)
        return (
            pltpu.make_async_copy(
                a_refs[d], t_buf.at[slot, pl.ds(2 * nb, na)], sem.at[slot, 0]
            ),
            pltpu.make_async_copy(b_refs[d], t_buf.at[slot, pl.ds(at, nb)], sem.at[slot, 1]),
            pltpu.make_async_copy(c_refs[d], t_buf.at[slot, pl.ds(other, nb)], sem.at[slot, 2]),
        )

    def weight_copy(index, slot):
        ref, column = w_refs[index]
        return pltpu.make_async_copy(
            ref.at[:, pl.ds(column, width)], w_buf.at[slot], sem.at[slot, 3]
        )

    def start(d, slot):
        for copy in token_copies(d, slot):
            copy.start()
        block = lax.rem(z + d, zn)
        across = lax.rem(block // 2 - y + yn, yn)
        side = lax.rem(block, 2)
        wanted = 2 * across + jnp.where(side == xl, 0, 1)
        for index in range(zn):
            @pl.when(wanted == index)
            def _():
                weight_copy(index, slot).start()

    def wait(d, slot):
        for copy in token_copies(d, slot):
            copy.wait()
        weight_copy(0, slot).wait()

    rows = t_buf.shape[1]
    steps = rows // ROWS
    start(0, 0)
    for d in range(zn):
        slot = d % 2
        if d + 1 < zn:
            start(d + 1, 1 - slot)
        wait(d, slot)

        def tile(i, carry):
            at = pl.ds(pl.multiple_of(i * ROWS, ROWS), ROWS)
            part = jnp.dot(
                t_buf[slot, at, :], w_buf[slot], preferred_element_type=jnp.float32
            )
            acc[at, :] = part if d == 0 else acc[at, :] + part
            return carry

        lax.fori_loop(0, steps, tile, 0)
    out = pltpu.make_async_copy(acc, out_ref, out_sem)
    out.start()
    out.wait()


def block_product(counts, a, b, c, weights, columns):
    zn, _, na, nb = counts
    rows, depth = na + 2 * nb, a[0].shape[1]
    width = 512

    def kernel(*refs):
        w = [(ref, at) for ref, at in zip(refs[3 * zn : 4 * zn], columns)]
        product_kernel(counts, *refs[: 3 * zn], *w, *refs[4 * zn :])

    anywhere = pl.BlockSpec(memory_space=pl.ANY)
    return pl.pallas_call(
        kernel,
        out_shape=jax.ShapeDtypeStruct((rows, width), jnp.float32),
        in_specs=[anywhere] * (4 * zn),
        out_specs=anywhere,
        scratch_shapes=[
            pltpu.VMEM((2, rows, depth), jnp.bfloat16),
            pltpu.VMEM((2, depth, width), jnp.bfloat16),
            pltpu.VMEM((rows, width), jnp.float32),
            pltpu.SemaphoreType.DMA((2, 4)),
            pltpu.SemaphoreType.DMA,
        ],
        compiler_params=pltpu.CompilerParams(vmem_limit_bytes=16 * 1024 * 1024),
        cost_estimate=pl.CostEstimate(
            flops=2 * rows * width * depth * zn,
            bytes_accessed=2 * zn * depth * (rows + width) + 4 * rows * width,
            transcendentals=0,
        ),
    )(*a, *b, *c, *weights)


def per_device(tokens, up_weight):
    core, xh = lax.axis_index("core"), lax.axis_index("xh")
    zn, yn = lax.axis_size("z"), lax.axis_size("y")
    rows, depth = tokens.shape
    nb = 3 * rows // 10
    na = rows - 2 * nb
    width = up_weight.shape[1] // 2

    def up(axis, a):
        return lax.ppermute(a, axis, ring(lax.axis_size(axis), 1))

    def down(axis, a):
        return lax.ppermute(a, axis, ring(lax.axis_size(axis), -1))

    def crossed(a, shift):
        pairs = [
            (2 * i + k, 2 * ((i + shift) % yn) + 1 - k) for i in range(yn) for k in range(2)
        ]
        return lax.ppermute(a, ("y", "core"), pairs)

    def quarter(parity, layer):
        return lax.dynamic_slice(
            up_weight, (parity * depth, layer * width), (depth, width)
        )

    b, c, a = {}, {}, {}
    b[0] = lax.dynamic_slice_in_dim(tokens, xh * nb, nb, 0)
    c[0] = lax.dynamic_slice_in_dim(tokens, (1 - xh) * nb, nb, 0)
    a[0] = tokens[2 * nb :]
    mine, given, far = quarter(core, xh), quarter(1 - core, xh), quarter(1 - core, 1 - xh)

    b[-1], b[1] = up("z", b[0]), down("z", b[0])
    a[-1], a[1] = up("z", a[0]), down("z", a[0])
    b[-2], b[2] = up("z", b[-1]), down("z", b[1])
    a[-2], a[2] = up("z", a[-1]), down("z", a[1])
    b[-3], b[3] = up("z", b[-2]), down("z", b[2])
    a[-3], a[3] = up("z", a[-2]), down("z", a[2])
    b[4], a[4] = down("z", b[3]), up("z", a[-3])
    for d in (-1, 1, -2, 2, -3, 3, 4):
        c[d] = lax.ppermute(b[d], "xh", ring(2, 1))

    wa, wb, wo = {0: mine}, {}, {}
    wa[-1], wa[1] = up("y", mine), down("y", mine)
    wb[-1], wb[1] = crossed(given, 1), crossed(given, -1)
    near = lax.ppermute(mine, "xl", ring(2, 1))
    across = lax.ppermute(far, ("xl", "core", "xh"), [(i, 7 - i) for i in range(8)])
    wb[0] = lax.ppermute(given, "core", ring(2, 1))
    wo[0] = jnp.concatenate([near, across], 1)
    wo[-1], wo[1] = up("y", wo[0]), down("y", wo[0])
    wa[2], wb[2] = up("y", wa[-1]), up("y", wb[-1])
    wo[2] = down("y", wo[1])

    def turn(pieces, size):
        return [pieces[d if d in pieces else d - size] for d in range(size)]

    counts = (zn, yn, na, nb)
    tokens_in = [turn(t, zn) for t in (a, b, c)]
    wa, wb, wo = (turn(w, yn) for w in (wa, wb, wo))

    def mixed(first):
        return [w for pair in zip(first, wo) for w in pair]

    partner = block_product(counts, *tokens_in, mixed(wb), (0, width) * yn)
    swapped = lax.ppermute(partner, "core", ring(2, 1))
    own = block_product(counts, *tokens_in, mixed(wa), (0, 0) * yn)
    return (own + swapped).astype(jnp.bfloat16)


def solution(mesh):
    split = Mesh(
        mesh.devices.reshape(4, 2, mesh.shape["col"] // 2, 2, mesh.shape["layer"]), AXES
    )
    spec = P(("y", "xl"), ("z", "core"))
    return jax.shard_map(
        per_device,
        mesh=split,
        in_specs=(spec, spec),
        out_specs=P(("y", "xl"), ("z", "core", "xh")),
        check_vma=False,
    )
```

```python
import jax
import jax.numpy as jnp
from jax import lax
from jax.experimental import pallas as pl
from jax.experimental.pallas import tpu as pltpu
from jax.sharding import Mesh
from jax.sharding import PartitionSpec as P


AXES = ("y", "xl", "z", "core", "xh")


def ring(size, shift):
    return [(i, (i + shift) % size) for i in range(size)]


def block_product(counts, a, b, c, weights, columns):
    zn, yn, na, nb = counts
    rows, depth, width = na + 2 * nb, a[0].shape[1], weights[0].shape[1]

    def kernel(*refs):
        a_refs, b_refs, c_refs = refs[:zn], refs[zn : 2 * zn], refs[2 * zn : 3 * zn]
        w_refs = refs[3 * zn : 4 * zn]
        out_ref, w_buf, sem = refs[4 * zn :]
        y, xl, z, xh = (lax.axis_index(axis) for axis in ("y", "xl", "z", "xh"))
        at_b = pl.multiple_of(xh * nb, nb)
        at_c = pl.multiple_of((1 - xh) * nb, nb)

        def copy(index, slot):
            return pltpu.make_async_copy(
                w_refs[index].at[:, pl.ds(columns[index], width)], w_buf.at[slot], sem.at[slot]
            )

        def start(d, slot):
            block = lax.rem(z + d, zn)
            across = lax.rem(block // 2 - y + yn, yn)
            wanted = 2 * across + jnp.where(lax.rem(block, 2) == xl, 0, 1)
            for index in range(zn):
                @pl.when(wanted == index)
                def _():
                    copy(index, slot).start()

        start(0, 0)
        for d in range(zn):
            slot = d % 2
            if d + 1 < zn:
                start(d + 1, 1 - slot)
            copy(0, slot).wait()
            for ref, at, n in (
                (a_refs[d], 2 * nb, na),
                (b_refs[d], at_b, nb),
                (c_refs[d], at_c, nb),
            ):
                where = pl.ds(at, n)
                part = jnp.dot(ref[...], w_buf[slot], preferred_element_type=jnp.float32)
                out_ref[where, :] = part if d == 0 else out_ref[where, :] + part

    anywhere = pl.BlockSpec(memory_space=pl.ANY)
    vmem = pl.BlockSpec(memory_space=pltpu.VMEM)
    return pl.pallas_call(
        kernel,
        out_shape=jax.ShapeDtypeStruct((rows, width), jnp.float32),
        in_specs=[vmem] * (3 * zn) + [anywhere] * zn,
        out_specs=vmem,
        scratch_shapes=[
            pltpu.VMEM((2, depth, width), jnp.bfloat16),
            pltpu.SemaphoreType.DMA((2,)),
        ],
        compiler_params=pltpu.CompilerParams(vmem_limit_bytes=8 * 1024 * 1024),
        cost_estimate=pl.CostEstimate(
            flops=2 * rows * width * depth * zn,
            bytes_accessed=2 * zn * depth * (rows + width) + 4 * rows * width,
            transcendentals=0,
        ),
    )(*a, *b, *c, *weights)


def per_device(tokens, up_weight):
    core, xh = lax.axis_index("core"), lax.axis_index("xh")
    zn, yn = lax.axis_size("z"), lax.axis_size("y")
    rows, depth = tokens.shape
    nb = 3 * rows // 10
    na = rows - 2 * nb
    width = up_weight.shape[1] // 2

    def up(axis, a):
        return lax.ppermute(a, axis, ring(lax.axis_size(axis), 1))

    def down(axis, a):
        return lax.ppermute(a, axis, ring(lax.axis_size(axis), -1))

    def crossed(a, shift):
        pairs = [
            (2 * i + k, 2 * ((i + shift) % yn) + 1 - k) for i in range(yn) for k in range(2)
        ]
        return lax.ppermute(a, ("y", "core"), pairs)

    def quarter(parity, layer):
        return lax.dynamic_slice(
            up_weight, (parity * depth, layer * width), (depth, width)
        )

    b, c, a = {}, {}, {}
    b[0] = lax.dynamic_slice_in_dim(tokens, xh * nb, nb, 0)
    c[0] = lax.dynamic_slice_in_dim(tokens, (1 - xh) * nb, nb, 0)
    a[0] = tokens[2 * nb :]
    mine, given, far = quarter(core, xh), quarter(1 - core, xh), quarter(1 - core, 1 - xh)

    b[-1], b[1] = up("z", b[0]), down("z", b[0])
    a[-1], a[1] = up("z", a[0]), down("z", a[0])
    b[-2], b[2] = up("z", b[-1]), down("z", b[1])
    a[-2], a[2] = up("z", a[-1]), down("z", a[1])
    b[-3], b[3] = up("z", b[-2]), down("z", b[2])
    a[-3], a[3] = up("z", a[-2]), down("z", a[2])
    b[4], a[4] = down("z", b[3]), up("z", a[-3])
    for d in (-1, 1, -2, 2, -3, 3, 4):
        c[d] = lax.ppermute(b[d], "xh", ring(2, 1))

    wa, wb, wo = {0: mine}, {}, {}
    wa[-1], wa[1] = up("y", mine), down("y", mine)
    wb[-1], wb[1] = crossed(given, 1), crossed(given, -1)
    near = lax.ppermute(mine, "xl", ring(2, 1))
    across = lax.ppermute(far, ("xl", "core", "xh"), [(i, 7 - i) for i in range(8)])
    wb[0] = lax.ppermute(given, "core", ring(2, 1))
    wo[0] = jnp.concatenate([near, across], 1)
    wo[-1], wo[1] = up("y", wo[0]), down("y", wo[0])
    wide = up("y", jnp.concatenate([wa[-1], wb[-1]], 1))
    wa[2], wb[2] = wide, wide
    wo[2] = down("y", wo[1])

    def turn(pieces, size):
        return [pieces[d if d in pieces else d - size] for d in range(size)]

    counts = (zn, yn, na, nb)
    tokens_in = [turn(t, zn) for t in (a, b, c)]
    wa, wb, wo = (turn(w, yn) for w in (wa, wb, wo))

    def mixed(first):
        return [w for pair in zip(first, wo) for w in pair]

    at = [width if w is wide or i % 2 else 0 for i, w in enumerate(mixed(wb))]
    partner = block_product(counts, *tokens_in, mixed(wb), at)
    swapped = lax.ppermute(partner, "core", ring(2, 1))
    own = block_product(counts, *tokens_in, mixed(wa), (0, 0) * yn)
    return (own + swapped).astype(jnp.bfloat16)


def solution(mesh):
    split = Mesh(
        mesh.devices.reshape(4, 2, mesh.shape["col"] // 2, 2, mesh.shape["layer"]), AXES
    )
    spec = P(("y", "xl"), ("z", "core"))
    return jax.shard_map(
        per_device,
        mesh=split,
        in_specs=(spec, spec),
        out_specs=P(("y", "xl"), ("z", "core", "xh")),
        check_vma=False,
    )
```

```python
import jax
import jax.numpy as jnp
from jax import lax
from jax.experimental import pallas as pl
from jax.experimental.pallas import tpu as pltpu
from jax.sharding import Mesh
from jax.sharding import PartitionSpec as P


AXES = ("y", "xl", "z", "core", "xh")


def ring(size, shift):
    return [(i, (i + shift) % size) for i in range(size)]


def block_product(counts, a, b, c, c_rows, weights, columns):
    zn, yn, na, nb = counts
    rows, depth, width = na + 2 * nb, a[0].shape[1], weights[0].shape[1]

    def kernel(*refs):
        a_refs, b_refs, c_refs = refs[:zn], refs[zn : 2 * zn], refs[2 * zn : 3 * zn]
        w_refs = refs[3 * zn : 4 * zn]
        out_ref, w_buf, sem = refs[4 * zn :]
        y, xl, z, xh = (lax.axis_index(axis) for axis in ("y", "xl", "z", "xh"))
        at_b = pl.multiple_of(xh * nb, nb)
        at_c = pl.multiple_of((1 - xh) * nb, nb)

        def copy(index, slot):
            return pltpu.make_async_copy(
                w_refs[index].at[:, pl.ds(columns[index], width)], w_buf.at[slot], sem.at[slot]
            )

        def start(d, slot):
            block = lax.rem(z + d, zn)
            across = lax.rem(block // 2 - y + yn, yn)
            wanted = 2 * across + jnp.where(lax.rem(block, 2) == xl, 0, 1)
            for index in range(zn):
                @pl.when(wanted == index)
                def _():
                    copy(index, slot).start()

        start(0, 0)
        for d in range(zn):
            slot = d % 2
            if d + 1 < zn:
                start(d + 1, 1 - slot)
            copy(0, slot).wait()
            for ref, first, at, n in (
                (a_refs[d], 0, 2 * nb, na),
                (b_refs[d], 0, at_b, nb),
                (c_refs[d], c_rows[d], at_c, nb),
            ):
                where = pl.ds(at, n)
                part = jnp.dot(
                    ref[first : first + n, :], w_buf[slot], preferred_element_type=jnp.float32
                )
                out_ref[where, :] = part if d == 0 else out_ref[where, :] + part

    anywhere = pl.BlockSpec(memory_space=pl.ANY)
    vmem = pl.BlockSpec(memory_space=pltpu.VMEM)
    return pl.pallas_call(
        kernel,
        out_shape=jax.ShapeDtypeStruct((rows, width), jnp.float32),
        in_specs=[vmem] * (3 * zn) + [anywhere] * zn,
        out_specs=vmem,
        scratch_shapes=[
            pltpu.VMEM((2, depth, width), jnp.bfloat16),
            pltpu.SemaphoreType.DMA((2,)),
        ],
        compiler_params=pltpu.CompilerParams(vmem_limit_bytes=8 * 1024 * 1024),
        cost_estimate=pl.CostEstimate(
            flops=2 * rows * width * depth * zn,
            bytes_accessed=2 * zn * depth * (rows + width) + 4 * rows * width,
            transcendentals=0,
        ),
    )(*a, *b, *c, *weights)


def per_device(tokens, up_weight):
    core, xh = lax.axis_index("core"), lax.axis_index("xh")
    zn, yn = lax.axis_size("z"), lax.axis_size("y")
    rows, depth = tokens.shape
    nb = 11 * rows // 40
    na = rows - 2 * nb
    width = up_weight.shape[1] // 2

    def up(axis, a):
        return lax.ppermute(a, axis, ring(lax.axis_size(axis), 1))

    def down(axis, a):
        return lax.ppermute(a, axis, ring(lax.axis_size(axis), -1))

    def crossed(a, shift):
        pairs = [
            (2 * i + k, 2 * ((i + shift) % yn) + 1 - k) for i in range(yn) for k in range(2)
        ]
        return lax.ppermute(a, ("y", "core"), pairs)

    def quarter(parity, layer):
        return lax.dynamic_slice(
            up_weight, (parity * depth, layer * width), (depth, width)
        )

    b, c, a = {}, {}, {}
    b[0] = lax.dynamic_slice_in_dim(tokens, xh * nb, nb, 0)
    c[0] = lax.dynamic_slice_in_dim(tokens, (1 - xh) * nb, nb, 0)
    a[0] = tokens[2 * nb :]
    mine, given, far = quarter(core, xh), quarter(1 - core, xh), quarter(1 - core, 1 - xh)

    b[-1], b[1] = up("z", b[0]), down("z", b[0])
    a[-1], a[1] = up("z", a[0]), down("z", a[0])
    b[-2], b[2] = up("z", b[-1]), down("z", b[1])
    a[-2], a[2] = up("z", a[-1]), down("z", a[1])
    b[-3], b[3] = up("z", b[-2]), down("z", b[2])
    a[-3], a[3] = up("z", a[-2]), down("z", a[2])
    b[4], a[4] = down("z", b[3]), up("z", a[-3])
    for d in (1, 2, 3):
        pair = lax.ppermute(jnp.concatenate([b[-d], b[d]], 0), "xh", ring(2, 1))
        c[-d], c[d] = (pair, 0), (pair, nb)
    c[0], c[4] = (c[0], 0), (lax.ppermute(b[4], "xh", ring(2, 1)), 0)

    wa, wb, wo = {0: mine}, {}, {}
    wa[-1], wa[1] = up("y", mine), down("y", mine)
    wb[-1], wb[1] = crossed(given, 1), crossed(given, -1)
    near = lax.ppermute(mine, "xl", ring(2, 1))
    across = lax.ppermute(far, ("xl", "core", "xh"), [(i, 7 - i) for i in range(8)])
    wb[0] = lax.ppermute(given, "core", ring(2, 1))
    wo[0] = jnp.concatenate([near, across], 1)
    wo[-1], wo[1] = up("y", wo[0]), down("y", wo[0])
    wide = up("y", jnp.concatenate([wa[-1], wb[-1]], 1))
    wa[2], wb[2] = wide, wide
    wo[2] = down("y", wo[1])

    def turn(pieces, size):
        return [pieces[d if d in pieces else d - size] for d in range(size)]

    counts = (zn, yn, na, nb)
    a, b, c = (turn(t, zn) for t in (a, b, c))
    tokens_in = (a, b, [t[0] for t in c], [t[1] for t in c])
    wa, wb, wo = (turn(w, yn) for w in (wa, wb, wo))

    def mixed(first):
        return [w for pair in zip(first, wo) for w in pair]

    at = [width if w is wide or i % 2 else 0 for i, w in enumerate(mixed(wb))]
    partner = block_product(counts, *tokens_in, mixed(wb), at)
    swapped = lax.ppermute(partner, "core", ring(2, 1))
    own = block_product(counts, *tokens_in, mixed(wa), (0, 0) * yn)
    return (own + swapped).astype(jnp.bfloat16)


def solution(mesh):
    split = Mesh(
        mesh.devices.reshape(4, 2, mesh.shape["col"] // 2, 2, mesh.shape["layer"]), AXES
    )
    spec = P(("y", "xl"), ("z", "core"))
    return jax.shard_map(
        per_device,
        mesh=split,
        in_specs=(spec, spec),
        out_specs=P(("y", "xl"), ("z", "core", "xh")),
        check_vma=False,
    )
```

```python
import jax
import jax.numpy as jnp
from jax import lax
from jax.experimental import pallas as pl
from jax.experimental.pallas import tpu as pltpu
from jax.sharding import Mesh
from jax.sharding import PartitionSpec as P


AXES = ("y", "xl", "z", "core", "xh")
NEAR = (0, 1, 2, -1, -2)
LATE = (3, -3, 4)


def ring(size, shift):
    return [(i, (i + shift) % size) for i in range(size)]


VMEM = pl.BlockSpec(memory_space=pltpu.VMEM)


def room(shapes):
    return pl.pallas_call(
        lambda *refs: None,
        name="room",
        out_shape=[jax.ShapeDtypeStruct(shape, jnp.bfloat16) for shape in shapes],
        out_specs=[pl.BlockSpec(memory_space=pl.ANY)] * len(shapes),
    )()


def add_product(out_ref, tokens_ref, weight):
    rows = out_ref.shape[0]
    for first in range(0, rows, rows // 2):
        at = slice(first, first + rows // 2)
        out_ref[at, :] += jnp.dot(
            tokens_ref[at, :], weight, preferred_element_type=jnp.float32
        )


def met(d, zn, yn):
    block = lax.rem(lax.axis_index("z") + d + zn, zn)
    return lax.rem(block // 2 - lax.axis_index("y") + yn, yn), lax.rem(block, 2)


def call(kernel, rows, width, depth, blocks, args, aliases):
    return pl.pallas_call(
        kernel,
        out_shape=jax.ShapeDtypeStruct((rows, width), jnp.float32),
        in_specs=[VMEM] * len(args),
        out_specs=VMEM,
        input_output_aliases=aliases,
        compiler_params=pltpu.CompilerParams(vmem_limit_bytes=4 * 1024 * 1024),
        cost_estimate=pl.CostEstimate(
            flops=2 * rows * width * depth * blocks,
            bytes_accessed=2 * blocks * depth * (rows + width) + 8 * rows * width,
            transcendentals=0,
        ),
    )(*args)


def early_product(t_near, w_near, half, zn, yn):
    rows, depth = t_near.shape[1:]
    width = w_near.shape[2] // 2
    columns = slice(half * width, (half + 1) * width)

    def kernel(t_ref, w_ref, out_ref):
        out_ref[...] = jnp.zeros_like(out_ref)

        def block(i, carry):
            d = jnp.where(i <= 2, i, 2 - i)
            across, _ = met(d, zn, yn)

            @pl.when(across != yn // 2)
            def _():
                at = lax.rem(d + zn, zn)
                add_product(out_ref, t_ref.at[i], w_ref[at, :, columns])

            return carry

        lax.fori_loop(0, len(NEAR), block, 0)

    return call(kernel, rows, width, depth, len(NEAR), (t_near, w_near), {})


def final_product(total, t_near, t_late, w_near, w_late, half, zn, yn):
    rows, depth = t_near.shape[1:]
    width = w_near.shape[2] // 2
    columns = slice(half * width, (half + 1) * width)

    def kernel(total_ref, tn_ref, tl_ref, wn_ref, wl_ref, out_ref):
        def near(i, carry):
            across, side = met(jnp.where(i <= 2, i, 2 - i), zn, yn)

            @pl.when(across == yn // 2)
            def _():
                add_product(out_ref, tn_ref.at[i], wl_ref[side, :, columns])

            return carry

        def late(i, carry):
            d = jnp.where(i == 0, 3, jnp.where(i == 1, -3, 4))
            across, side = met(d, zn, yn)

            @pl.when(across != yn // 2)
            def _():
                add_product(out_ref, tl_ref.at[i], wn_ref[lax.rem(d + zn, zn), :, columns])

            @pl.when(across == yn // 2)
            def _():
                add_product(out_ref, tl_ref.at[i], wl_ref[side, :, columns])

            return carry

        lax.fori_loop(0, len(NEAR), near, 0)
        lax.fori_loop(0, len(LATE), late, 0)

    args = (total, t_near, t_late, w_near, w_late)
    return call(kernel, rows, width, depth, len(LATE), args, {0: 0})


def per_device(tokens, up_weight):
    y, xl, z, core, xh = (lax.axis_index(axis) for axis in AXES)
    zn, yn = lax.axis_size("z"), lax.axis_size("y")
    rows, depth = tokens.shape
    nb = 11 * rows // 40
    width = up_weight.shape[1] // 2

    def up(axis, a):
        return lax.ppermute(a, axis, ring(lax.axis_size(axis), 1))

    def down(axis, a):
        return lax.ppermute(a, axis, ring(lax.axis_size(axis), -1))

    def crossed(a, shift):
        pairs = [
            (2 * i + k, 2 * ((i + shift) % yn) + 1 - k) for i in range(yn) for k in range(2)
        ]
        return lax.ppermute(a, ("y", "core"), pairs)

    def quarter(parity, layer):
        return lax.dynamic_slice(
            up_weight, (parity * depth, layer * width), (depth, width)
        )

    b, c, a = {}, {}, {}
    b[0] = lax.dynamic_slice_in_dim(tokens, xh * nb, nb, 0)
    c[0] = lax.dynamic_slice_in_dim(tokens, (1 - xh) * nb, nb, 0)
    a[0] = tokens[2 * nb :]
    mine, given, far = quarter(core, xh), quarter(1 - core, xh), quarter(1 - core, 1 - xh)

    b[-1], b[1] = up("z", b[0]), down("z", b[0])
    a[-1], a[1] = up("z", a[0]), down("z", a[0])
    b[-2], b[2] = up("z", b[-1]), down("z", b[1])
    a[-2], a[2] = up("z", a[-1]), down("z", a[1])
    b[-3], b[3] = up("z", b[-2]), down("z", b[2])
    a[-3], a[3] = up("z", a[-2]), down("z", a[2])
    b[4], a[4] = down("z", b[3]), up("z", a[-3])
    for d in (1, 2, 3):
        pair = lax.ppermute(jnp.concatenate([b[-d], b[d]], 0), "xh", ring(2, 1))
        c[-d], c[d] = (pair, 0), (pair, nb)
    c[0], c[4] = (c[0], 0), (lax.ppermute(b[4], "xh", ring(2, 1)), 0)

    wa, wb, wo = {0: mine}, {}, {}
    wa[-1], wa[1] = up("y", mine), down("y", mine)
    wb[-1], wb[1] = crossed(given, 1), crossed(given, -1)
    near = lax.ppermute(mine, "xl", ring(2, 1))
    across = lax.ppermute(far, ("xl", "core", "xh"), [(i, 7 - i) for i in range(8)])
    wb[0] = lax.ppermute(given, "core", ring(2, 1))
    wo[0] = jnp.concatenate([near, across], 1)
    wo[-1], wo[1] = up("y", wo[0]), down("y", wo[0])
    wide = up("y", jnp.concatenate([wa[-1], wb[-1]], 1))
    wo[2] = down("y", wo[1])

    t_near, t_late, w_near, w_late = room(
        (
            (len(NEAR), rows, depth),
            (len(LATE), rows, depth),
            (zn, depth, 2 * width),
            (2, depth, 2 * width),
        )
    )

    def put(stack, piece, *at):
        return lax.dynamic_update_slice(stack, piece[None], at)

    def put_tokens(stack, order):
        for i, d in enumerate(order):
            pair, first = c[d]
            stack = put(stack, a[d], i, 2 * nb, 0)
            stack = put(stack, b[d], i, xh * nb, 0)
            stack = put(stack, pair[first : first + nb], i, (1 - xh) * nb, 0)
        return stack

    t_near, t_late = put_tokens(t_near, NEAR), put_tokens(t_late, LATE)
    for dy in (0, -1, 1):
        row = 2 * lax.rem(y + dy + yn, yn) - z + 2 * zn
        own, other = lax.rem(row + xl, zn), lax.rem(row + 1 - xl, zn)
        w_near = put(w_near, wa[dy], own, 0, 0)
        w_near = put(w_near, wb[dy], own, 0, width)
        w_near = put(w_near, wo[dy], other, 0, 0)
    w_late = put(w_late, wide, xl, 0, 0)
    w_late = put(w_late, wo[2], 1 - xl, 0, 0)

    total = {}
    for half in (1, 0):
        total[half] = early_product(t_near, w_near, half, zn, yn)
    rest = (t_near, t_late, w_near, w_late)
    partner = final_product(total[1], *rest, 1, zn, yn)
    swapped = lax.ppermute(partner, "core", ring(2, 1))
    own = final_product(total[0], *rest, 0, zn, yn)
    return (own + swapped).astype(jnp.bfloat16)


def solution(mesh):
    split = Mesh(
        mesh.devices.reshape(4, 2, mesh.shape["col"] // 2, 2, mesh.shape["layer"]), AXES
    )
    spec = P(("y", "xl"), ("z", "core"))
    return jax.shard_map(
        per_device,
        mesh=split,
        in_specs=(spec, spec),
        out_specs=P(("y", "xl"), ("z", "core", "xh")),
        check_vma=False,
    )
```

```python
import functools

import jax
import jax.numpy as jnp
from jax import lax
from jax.experimental import pallas as pl
from jax.experimental.pallas import tpu as pltpu
from jax.sharding import Mesh
from jax.sharding import PartitionSpec as P


AXES = ("y", "xl", "z", "core", "xh")
NEAR = (0, 1, 2, -1, -2)
LATE = (3, -3, 4)


def ring(size, shift):
    return [(i, (i + shift) % size) for i in range(size)]


VMEM = pl.BlockSpec(memory_space=pltpu.VMEM)
ANYWHERE = pl.BlockSpec(memory_space=pl.ANY)


def meets(d, zn, yn):
    y, xl, z = (lax.axis_index(axis) for axis in ("y", "xl", "z"))
    block = lax.rem(z + d + zn, zn)
    across = lax.rem(block // 2 - y + yn, yn)
    return across, 2 * across + jnp.where(lax.rem(block, 2) == xl, 0, 1)


def places(rows, nb):
    xh = lax.axis_index("xh")
    return (
        pl.ds(2 * nb, rows - 2 * nb),
        pl.ds(pl.multiple_of(xh * nb, nb), nb),
        pl.ds(pl.multiple_of((1 - xh) * nb, nb), nb),
    )


def call(kernel, out_shape, blocks, tokens, weights, extra, scratch):
    rows, width = out_shape[-2:]
    depth = weights[0].shape[0]
    parts = [part for block in tokens for part, _ in block]
    return pl.pallas_call(
        kernel,
        out_shape=jax.ShapeDtypeStruct(out_shape, jnp.float32),
        in_specs=[VMEM] * (len(extra) + len(parts)) + [ANYWHERE] * len(weights),
        out_specs=VMEM,
        scratch_shapes=[pltpu.VMEM((2, depth, width), jnp.bfloat16), pltpu.SemaphoreType.DMA((2,))]
        + scratch,
        compiler_params=pltpu.CompilerParams(vmem_limit_bytes=8 * 1024 * 1024),
        cost_estimate=pl.CostEstimate(
            flops=2 * rows * width * depth * blocks,
            bytes_accessed=2 * blocks * depth * (rows + width) + 4 * rows * width,
            transcendentals=0,
        ),
    )(*extra, *parts, *weights)


def early_product(tokens, near_weights, rows, nb, zn, yn):
    width = near_weights[0][0][0].shape[1]
    arrays = [w for half in near_weights for w, _ in half]
    known = (0, 1, 2, 3, 2 * yn - 2, 2 * yn - 1)

    def kernel(*refs):
        parts, w_refs = refs[: 3 * len(NEAR)], refs[3 * len(NEAR) : -3]
        out_ref, w_buf, sem = refs[-3:]
        at = places(rows, nb)

        def copy(half, i, slot):
            return pltpu.make_async_copy(
                w_refs[6 * half + i].at[:, pl.ds(near_weights[half][i][1], width)],
                w_buf.at[slot],
                sem.at[slot],
            )

        def start(turn, d, slot):
            _, index = meets(d, zn, yn)
            for half in range(2):
                for i, number in enumerate(known):
                    @pl.when(jnp.logical_and(turn == half, index == number))
                    def _():
                        copy(half, i, slot).start()

        def both(turn, carry):
            out_ref[turn] = jnp.zeros((rows, width), jnp.float32)
            start(turn, NEAR[0], 0)
            for j, d in enumerate(NEAR):
                slot = j % 2
                if j + 1 < len(NEAR):
                    start(turn, NEAR[j + 1], 1 - slot)

                @pl.when(meets(d, zn, yn)[0] != yn // 2)
                def _():
                    copy(0, 0, slot).wait()
                    for ref, (part, first), where in zip(parts[3 * j : 3 * j + 3], tokens[j], at):
                        out_ref[turn, where, :] += jnp.dot(
                            ref[first : first + where.size, :],
                            w_buf[slot],
                            preferred_element_type=jnp.float32,
                        )

            return carry

        lax.fori_loop(0, 2, both, 0)

    return call(kernel, (2, rows, width), 6, tokens, arrays, [], [])


def final_product(half, total, late_tokens, near_tokens, weights, rows, nb, zn, yn):
    depth, width = weights[0][0].shape[0], total.shape[2]
    tokens = late_tokens + near_tokens
    late = len(LATE)

    def kernel(total_ref, *refs):
        parts, w_refs = refs[: 3 * len(tokens)], refs[3 * len(tokens) : -5]
        out_ref, w_buf, w_sem, t_buf, t_sem = refs[-5:]
        at = places(rows, nb)

        def weight_copy(i, slot):
            return pltpu.make_async_copy(
                w_refs[i].at[:, pl.ds(weights[i][1], width)], w_buf.at[slot], w_sem.at[slot]
            )

        def start_weight(index, slot, wanted):
            for i in range(len(weights)):
                @pl.when(jnp.logical_and(wanted, index == i))
                def _():
                    weight_copy(i, slot).start()

        def token_copies(j, slot):
            return [
                pltpu.make_async_copy(
                    ref.at[pl.ds(first, where.size)], t_buf.at[slot, where], t_sem.at[slot, k]
                )
                for k, (ref, (_, first), where) in enumerate(
                    zip(parts[3 * j : 3 * j + 3], tokens[j], at)
                )
            ]

        start_weight(meets(LATE[0], zn, yn)[1], 0, True)
        found, side = jnp.int32(0), [jnp.int32(0)] * 2
        for j, d in enumerate(NEAR):
            across, index = meets(d, zn, yn)
            for slot in range(2):
                here = jnp.logical_and(across == yn // 2, found == slot)
                side[slot] = jnp.where(here, index, side[slot])

                @pl.when(here)
                def _():
                    for copy in token_copies(late + j, slot):
                        copy.start()
            found = found + jnp.where(across == yn // 2, 1, 0)

        for j in range(late):
            slot = j % 2
            if j + 1 < late:
                start_weight(meets(LATE[j + 1], zn, yn)[1], 1 - slot, True)
            else:
                start_weight(side[0], 1 - slot, found > 0)
            weight_copy(0, slot).wait()
            for ref, (_, first), where in zip(parts[3 * j : 3 * j + 3], tokens[j], at):
                before = total_ref[half, where, :] if j == 0 else out_ref[where, :]
                out_ref[where, :] = before + jnp.dot(
                    ref[first : first + where.size, :],
                    w_buf[slot],
                    preferred_element_type=jnp.float32,
                )

        def rest(k, carry):
            slot = lax.rem(late + k, 2)

            @pl.when(jnp.logical_and(k == 0, found > 1))
            def _():
                start_weight(side[1], 1 - late % 2, True)

            weight_copy(0, slot).wait()
            for copy in token_copies(late, k):
                copy.wait()
            for first in range(0, rows, rows // 2):
                where = slice(first, first + rows // 2)
                out_ref[where, :] += jnp.dot(
                    t_buf[k, where, :], w_buf[slot], preferred_element_type=jnp.float32
                )
            return carry

        lax.fori_loop(0, found, rest, 0)

    scratch = [pltpu.VMEM((2, rows, depth), jnp.bfloat16), pltpu.SemaphoreType.DMA((2, 3))]
    arrays = [w for w, _ in weights]
    return call(kernel, (rows, width), 4, tokens, arrays, [total], scratch)


def per_device(tokens, up_weight):
    _, _, _, core, xh = (lax.axis_index(axis) for axis in AXES)
    zn, yn = lax.axis_size("z"), lax.axis_size("y")
    rows, depth = tokens.shape
    nb = 11 * rows // 40
    width = up_weight.shape[1] // 2

    def up(axis, a):
        return lax.ppermute(a, axis, ring(lax.axis_size(axis), 1))

    def down(axis, a):
        return lax.ppermute(a, axis, ring(lax.axis_size(axis), -1))

    def crossed(a, shift):
        pairs = [
            (2 * i + k, 2 * ((i + shift) % yn) + 1 - k) for i in range(yn) for k in range(2)
        ]
        return lax.ppermute(a, ("y", "core"), pairs)

    def quarter(parity, layer):
        return lax.dynamic_slice(
            up_weight, (parity * depth, layer * width), (depth, width)
        )

    b, c, a = {}, {}, {}
    b[0] = lax.dynamic_slice_in_dim(tokens, xh * nb, nb, 0)
    c[0] = lax.dynamic_slice_in_dim(tokens, (1 - xh) * nb, nb, 0)
    a[0] = tokens[2 * nb :]
    mine, given, far = quarter(core, xh), quarter(1 - core, xh), quarter(1 - core, 1 - xh)

    b[-1], b[1] = up("z", b[0]), down("z", b[0])
    a[-1], a[1] = up("z", a[0]), down("z", a[0])
    b[-2], b[2] = up("z", b[-1]), down("z", b[1])
    a[-2], a[2] = up("z", a[-1]), down("z", a[1])
    b[-3], b[3] = up("z", b[-2]), down("z", b[2])
    a[-3], a[3] = up("z", a[-2]), down("z", a[2])
    b[4], a[4] = down("z", b[3]), up("z", a[-3])
    for d in (1, 2, 3):
        pair = lax.ppermute(jnp.concatenate([b[-d], b[d]], 0), "xh", ring(2, 1))
        c[-d], c[d] = (pair, 0), (pair, nb)
    c[0], c[4] = (c[0], 0), (lax.ppermute(b[4], "xh", ring(2, 1)), 0)

    wa, wb, wo = {0: mine}, {}, {}
    wa[-1], wa[1] = up("y", mine), down("y", mine)
    wb[-1], wb[1] = crossed(given, 1), crossed(given, -1)
    near = lax.ppermute(mine, "xl", ring(2, 1))
    across = lax.ppermute(far, ("xl", "core", "xh"), [(i, 7 - i) for i in range(8)])
    wb[0] = lax.ppermute(given, "core", ring(2, 1))
    wo[0] = jnp.concatenate([near, across], 1)
    wo[-1], wo[1] = up("y", wo[0]), down("y", wo[0])
    wide = jnp.concatenate([wa[-1], wb[-1]], 1)
    wide = up("y", wide)
    wo[2] = down("y", wo[1])

    def block(d):
        return [(a[d], 0), (b[d], 0), c[d]]

    near, late = [block(d) for d in NEAR], [block(d) for d in LATE]

    def weights(half, distances):
        listed = []
        for dy in distances:
            own = (wide, half * width) if dy == 2 else ((wb if half else wa)[dy], 0)
            listed += [own, (wo[dy], half * width)]
        return listed

    sizes = (rows, nb, zn, yn)
    total = early_product(near, [weights(half, (0, 1, -1)) for half in range(2)], *sizes)
    rest = [
        functools.partial(
            final_product, half, total, late, near, weights(half, (0, 1, 2, -1)), *sizes
        )
        for half in range(2)
    ]
    swapped = lax.ppermute(rest[1](), "core", ring(2, 1))
    return (rest[0]() + swapped).astype(jnp.bfloat16)


def solution(mesh):
    split = Mesh(
        mesh.devices.reshape(4, 2, mesh.shape["col"] // 2, 2, mesh.shape["layer"]), AXES
    )
    spec = P(("y", "xl"), ("z", "core"))
    return jax.shard_map(
        per_device,
        mesh=split,
        in_specs=(spec, spec),
        out_specs=P(("y", "xl"), ("z", "core", "xh")),
        check_vma=False,
    )
```

```python
import functools

import jax
import jax.numpy as jnp
from jax import lax
from jax.experimental import pallas as pl
from jax.experimental.pallas import tpu as pltpu
from jax.sharding import Mesh
from jax.sharding import PartitionSpec as P


AXES = ("y", "xl", "z", "core", "xh")
NEAR = (0, 1, 2, -1, -2)
MIDDLE = (3, -3)
LATE = (4,)


def ring(size, shift):
    return [(i, (i + shift) % size) for i in range(size)]


VMEM = pl.BlockSpec(memory_space=pltpu.VMEM)
ANYWHERE = pl.BlockSpec(memory_space=pl.ANY)


def meets(d, zn, yn):
    y, xl, z = (lax.axis_index(axis) for axis in ("y", "xl", "z"))
    block = lax.rem(z + d + zn, zn)
    across = lax.rem(block // 2 - y + yn, yn)
    return across, 2 * across + jnp.where(lax.rem(block, 2) == xl, 0, 1)


def places(rows, nb):
    xh = lax.axis_index("xh")
    return (
        pl.ds(2 * nb, rows - 2 * nb),
        pl.ds(pl.multiple_of(xh * nb, nb), nb),
        pl.ds(pl.multiple_of((1 - xh) * nb, nb), nb),
    )


def call(kernel, out_shape, blocks, tokens, weights, extra, scratch, aliases):
    rows, width = out_shape[-2:]
    depth = weights[0].shape[0]
    parts = [part for block in tokens for part, _ in block]
    return pl.pallas_call(
        kernel,
        out_shape=jax.ShapeDtypeStruct(out_shape, jnp.float32),
        in_specs=[VMEM] * (len(extra) + len(parts)) + [ANYWHERE] * len(weights),
        out_specs=VMEM,
        input_output_aliases=aliases,
        scratch_shapes=[pltpu.VMEM((2, depth, width), jnp.bfloat16), pltpu.SemaphoreType.DMA((2,))]
        + scratch,
        compiler_params=pltpu.CompilerParams(vmem_limit_bytes=8 * 1024 * 1024),
        cost_estimate=pl.CostEstimate(
            flops=2 * rows * width * depth * blocks,
            bytes_accessed=2 * blocks * depth * (rows + width) + 4 * rows * width,
            transcendentals=0,
        ),
    )(*extra, *parts, *weights)


def early_product(order, total, tokens, near_weights, rows, nb, zn, yn):
    width = near_weights[0][0][0].shape[1]
    arrays = [w for half in near_weights for w, _ in half]
    known = (0, 1, 2, 3, 2 * yn - 2, 2 * yn - 1)
    totals = [] if total is None else [total]

    def kernel(*refs):
        refs, (out_ref, w_buf, sem) = refs[len(totals) : -3], refs[-3:]
        parts, w_refs = refs[: 3 * len(order)], refs[3 * len(order) :]
        at = places(rows, nb)

        def copy(half, i, slot):
            return pltpu.make_async_copy(
                w_refs[6 * half + i].at[:, pl.ds(near_weights[half][i][1], width)],
                w_buf.at[slot],
                sem.at[slot],
            )

        def start(turn, d, slot):
            _, index = meets(d, zn, yn)
            for half in range(2):
                for i, number in enumerate(known):
                    @pl.when(jnp.logical_and(turn == half, index == number))
                    def _():
                        copy(half, i, slot).start()

        def both(turn, carry):
            if total is None:
                out_ref[turn] = jnp.zeros((rows, width), jnp.float32)
            start(turn, order[0], 0)
            for j, d in enumerate(order):
                slot = j % 2
                if j + 1 < len(order):
                    start(turn, order[j + 1], 1 - slot)

                @pl.when(meets(d, zn, yn)[0] != yn // 2)
                def _():
                    copy(0, 0, slot).wait()
                    for ref, (part, first), where in zip(parts[3 * j : 3 * j + 3], tokens[j], at):
                        out_ref[turn, where, :] += jnp.dot(
                            ref[first : first + where.size, :],
                            w_buf[slot],
                            preferred_element_type=jnp.float32,
                        )

            return carry

        lax.fori_loop(0, 2, both, 0)

    blocks = 2 * len(order)
    aliases = {i: 0 for i in range(len(totals))}
    return call(kernel, (2, rows, width), blocks, tokens, arrays, totals, [], aliases)


def final_product(half, total, late_tokens, near_tokens, weights, rows, nb, zn, yn):
    depth, width = weights[0][0].shape[0], total.shape[2]
    tokens = late_tokens + near_tokens
    late = len(LATE)

    def kernel(total_ref, *refs):
        parts, w_refs = refs[: 3 * len(tokens)], refs[3 * len(tokens) : -5]
        out_ref, w_buf, w_sem, t_buf, t_sem = refs[-5:]
        at = places(rows, nb)

        def weight_copy(i, slot):
            return pltpu.make_async_copy(
                w_refs[i].at[:, pl.ds(weights[i][1], width)], w_buf.at[slot], w_sem.at[slot]
            )

        def start_weight(index, slot, wanted):
            for i in range(len(weights)):
                @pl.when(jnp.logical_and(wanted, index == i))
                def _():
                    weight_copy(i, slot).start()

        def token_copies(j, slot):
            return [
                pltpu.make_async_copy(
                    ref.at[pl.ds(first, where.size)], t_buf.at[slot, where], t_sem.at[slot, k]
                )
                for k, (ref, (_, first), where) in enumerate(
                    zip(parts[3 * j : 3 * j + 3], tokens[j], at)
                )
            ]

        start_weight(meets(LATE[0], zn, yn)[1], 0, True)
        found, side = jnp.int32(0), [jnp.int32(0)] * 2
        for j, d in enumerate(NEAR + MIDDLE):
            across, index = meets(d, zn, yn)
            for slot in range(2):
                here = jnp.logical_and(across == yn // 2, found == slot)
                side[slot] = jnp.where(here, index, side[slot])

                @pl.when(here)
                def _():
                    for copy in token_copies(late + j, slot):
                        copy.start()
            found = found + jnp.where(across == yn // 2, 1, 0)

        for j in range(late):
            slot = j % 2
            if j + 1 < late:
                start_weight(meets(LATE[j + 1], zn, yn)[1], 1 - slot, True)
            else:
                start_weight(side[0], 1 - slot, found > 0)
            weight_copy(0, slot).wait()
            for ref, (_, first), where in zip(parts[3 * j : 3 * j + 3], tokens[j], at):
                before = total_ref[half, where, :] if j == 0 else out_ref[where, :]
                out_ref[where, :] = before + jnp.dot(
                    ref[first : first + where.size, :],
                    w_buf[slot],
                    preferred_element_type=jnp.float32,
                )

        def rest(k, carry):
            slot = lax.rem(late + k, 2)

            @pl.when(jnp.logical_and(k == 0, found > 1))
            def _():
                start_weight(side[1], 1 - late % 2, True)

            weight_copy(0, slot).wait()
            for copy in token_copies(late, k):
                copy.wait()
            for first in range(0, rows, rows // 2):
                where = slice(first, first + rows // 2)
                out_ref[where, :] += jnp.dot(
                    t_buf[k, where, :], w_buf[slot], preferred_element_type=jnp.float32
                )
            return carry

        lax.fori_loop(0, found, rest, 0)

    scratch = [pltpu.VMEM((2, rows, depth), jnp.bfloat16), pltpu.SemaphoreType.DMA((2, 3))]
    arrays = [w for w, _ in weights]
    return call(kernel, (rows, width), 3, tokens, arrays, [total], scratch, {})


def per_device(tokens, up_weight):
    _, _, _, core, xh = (lax.axis_index(axis) for axis in AXES)
    zn, yn = lax.axis_size("z"), lax.axis_size("y")
    rows, depth = tokens.shape
    nb = rows // 4
    width = up_weight.shape[1] // 2

    def up(axis, a):
        return lax.ppermute(a, axis, ring(lax.axis_size(axis), 1))

    def down(axis, a):
        return lax.ppermute(a, axis, ring(lax.axis_size(axis), -1))

    def crossed(a, shift):
        pairs = [
            (2 * i + k, 2 * ((i + shift) % yn) + 1 - k) for i in range(yn) for k in range(2)
        ]
        return lax.ppermute(a, ("y", "core"), pairs)

    def quarter(parity, layer):
        return lax.dynamic_slice(
            up_weight, (parity * depth, layer * width), (depth, width)
        )

    b, c, a = {}, {}, {}
    b[0] = lax.dynamic_slice_in_dim(tokens, xh * nb, nb, 0)
    c[0] = lax.dynamic_slice_in_dim(tokens, (1 - xh) * nb, nb, 0)
    a[0] = tokens[2 * nb :]
    mine, given, far = quarter(core, xh), quarter(1 - core, xh), quarter(1 - core, 1 - xh)

    b[-1], b[1] = up("z", b[0]), down("z", b[0])
    a[-1], a[1] = up("z", a[0]), down("z", a[0])
    b[-2], b[2] = up("z", b[-1]), down("z", b[1])
    a[-2], a[2] = up("z", a[-1]), down("z", a[1])
    b[-3], b[3] = up("z", b[-2]), down("z", b[2])
    a[-3], a[3] = up("z", a[-2]), down("z", a[2])
    b[4], a[4] = down("z", b[3]), up("z", a[-3])
    for d in (1, 2, 3):
        pair = lax.ppermute(jnp.concatenate([b[-d], b[d]], 0), "xh", ring(2, 1))
        c[-d], c[d] = (pair, 0), (pair, nb)
    c[0], c[4] = (c[0], 0), (lax.ppermute(b[4], "xh", ring(2, 1)), 0)

    wa, wb, wo = {0: mine}, {}, {}
    wa[-1], wa[1] = up("y", mine), down("y", mine)
    wb[-1], wb[1] = crossed(given, 1), crossed(given, -1)
    near = lax.ppermute(mine, "xl", ring(2, 1))
    across = lax.ppermute(far, ("xl", "core", "xh"), [(i, 7 - i) for i in range(8)])
    wb[0] = lax.ppermute(given, "core", ring(2, 1))
    wo[0] = jnp.concatenate([near, across], 1)
    wo[-1], wo[1] = up("y", wo[0]), down("y", wo[0])
    wide = jnp.concatenate([wa[-1], wb[-1]], 1)
    wide = up("y", wide)
    wo[2] = down("y", wo[1])

    def block(d):
        return [(a[d], 0), (b[d], 0), c[d]]

    near, middle, late = ([block(d) for d in order] for order in (NEAR, MIDDLE, LATE))

    def weights(half, distances):
        listed = []
        for dy in distances:
            own = (wide, half * width) if dy == 2 else ((wb if half else wa)[dy], 0)
            listed += [own, (wo[dy], half * width)]
        return listed

    sizes = (rows, nb, zn, yn)
    near_weights = [weights(half, (0, 1, -1)) for half in range(2)]
    total = early_product(NEAR, None, near, near_weights, *sizes)
    total = early_product(MIDDLE, total, middle, near_weights, *sizes)
    rest = [
        functools.partial(
            final_product, half, total, late, near + middle, weights(half, (0, 1, 2, -1)), *sizes
        )
        for half in range(2)
    ]
    swapped = lax.ppermute(rest[1](), "core", ring(2, 1))
    return (rest[0]() + swapped).astype(jnp.bfloat16)


def solution(mesh):
    split = Mesh(
        mesh.devices.reshape(4, 2, mesh.shape["col"] // 2, 2, mesh.shape["layer"]), AXES
    )
    spec = P(("y", "xl"), ("z", "core"))
    return jax.shard_map(
        per_device,
        mesh=split,
        in_specs=(spec, spec),
        out_specs=P(("y", "xl"), ("z", "core", "xh")),
        check_vma=False,
    )
```

```python
import jax
import jax.numpy as jnp
from jax import lax
from jax.experimental import pallas as pl
from jax.experimental.pallas import tpu as pltpu
from jax.sharding import Mesh
from jax.sharding import PartitionSpec as P


AXES = ("y", "xl", "z", "core", "xh")
FIRST = (0, 1, -1)
SECOND = (2, -2)
THIRD = (3, -3)
LATE = (4,)


def ring(size, shift):
    return [(i, (i + shift) % size) for i in range(size)]


VMEM = pl.BlockSpec(memory_space=pltpu.VMEM)
ANYWHERE = pl.BlockSpec(memory_space=pl.ANY)


def meets(d, zn, yn):
    y, xl, z = (lax.axis_index(axis) for axis in ("y", "xl", "z"))
    block = lax.rem(z + d + zn, zn)
    across = lax.rem(block // 2 - y + yn, yn)
    return across, 2 * across + jnp.where(lax.rem(block, 2) == xl, 0, 1)


def places(rows, nb):
    xh = lax.axis_index("xh")
    return (
        pl.ds(2 * nb, rows - 2 * nb),
        pl.ds(pl.multiple_of(xh * nb, nb), nb),
        pl.ds(pl.multiple_of((1 - xh) * nb, nb), nb),
    )


def call(kernel, out_shape, blocks, tokens, weights, extra, scratch, aliases):
    rows, width = out_shape[-2:]
    depth = weights[0].shape[0]
    parts = [part for block in tokens for part, _ in block]
    return pl.pallas_call(
        kernel,
        out_shape=jax.ShapeDtypeStruct(out_shape, jnp.float32),
        in_specs=[VMEM] * (len(extra) + len(parts)) + [ANYWHERE] * len(weights),
        out_specs=VMEM,
        input_output_aliases=aliases,
        scratch_shapes=[pltpu.VMEM((2, depth, width), jnp.bfloat16), pltpu.SemaphoreType.DMA((2,))]
        + scratch,
        compiler_params=pltpu.CompilerParams(vmem_limit_bytes=8 * 1024 * 1024),
        cost_estimate=pl.CostEstimate(
            flops=2 * rows * width * depth * blocks,
            bytes_accessed=2 * blocks * depth * (rows + width) + 4 * rows * width,
            transcendentals=0,
        ),
    )(*extra, *parts, *weights)


def early_product(order, total, tokens, near_weights, rows, nb, zn, yn):
    width = near_weights[0][0][0].shape[1]
    arrays = [w for half in near_weights for w, _ in half]
    known = (0, 1, 2, 3, 2 * yn - 2, 2 * yn - 1)
    totals = [] if total is None else [total]

    def kernel(*refs):
        refs, (out_ref, w_buf, sem) = refs[len(totals) : -3], refs[-3:]
        parts, w_refs = refs[: 3 * len(order)], refs[3 * len(order) :]
        at = places(rows, nb)

        def copy(half, i, slot):
            return pltpu.make_async_copy(
                w_refs[6 * half + i].at[:, pl.ds(near_weights[half][i][1], width)],
                w_buf.at[slot],
                sem.at[slot],
            )

        def start(turn, d, slot):
            _, index = meets(d, zn, yn)
            for half in range(2):
                for i, number in enumerate(known):
                    @pl.when(jnp.logical_and(turn == half, index == number))
                    def _():
                        copy(half, i, slot).start()

        def both(turn, carry):
            if total is None:
                out_ref[turn] = jnp.zeros((rows, width), jnp.float32)
            start(turn, order[0], 0)
            for j, d in enumerate(order):
                slot = j % 2
                if j + 1 < len(order):
                    start(turn, order[j + 1], 1 - slot)

                @pl.when(meets(d, zn, yn)[0] != yn // 2)
                def _():
                    copy(0, 0, slot).wait()
                    for ref, (part, first), where in zip(parts[3 * j : 3 * j + 3], tokens[j], at):
                        out_ref[turn, where, :] += jnp.dot(
                            ref[first : first + where.size, :],
                            w_buf[slot],
                            preferred_element_type=jnp.float32,
                        )

            return carry

        lax.fori_loop(0, 2, both, 0)

    blocks = 2 * len(order)
    aliases = {i: 0 for i in range(len(totals))}
    return call(kernel, (2, rows, width), blocks, tokens, arrays, totals, [], aliases)


def final_product(half, used, total, late_tokens, near_tokens, weights, rows, nb, zn, yn):
    depth, width = weights[0][0].shape[0], total.shape[2]
    tokens = [[block[part] for part in used] for block in late_tokens + near_tokens]
    late, n = len(LATE), len(used)
    base = 2 * nb if used == (0,) else 0
    wanted_rows = sum((rows - 2 * nb, nb, nb)[part] for part in used)

    def kernel(total_ref, *refs):
        parts, w_refs = refs[: n * len(tokens)], refs[n * len(tokens) : -5]
        out_ref, w_buf, w_sem, t_buf, t_sem = refs[-5:]
        from_total = [places(rows, nb)[part] for part in used]
        at = [pl.ds(0, where.size) if base else where for where in from_total]

        def weight_copy(i, slot):
            return pltpu.make_async_copy(
                w_refs[i].at[:, pl.ds(weights[i][1], width)], w_buf.at[slot], w_sem.at[slot]
            )

        def start_weight(index, slot, wanted):
            for i in range(len(weights)):
                @pl.when(jnp.logical_and(wanted, index == i))
                def _():
                    weight_copy(i, slot).start()

        def token_copies(j, slot):
            return [
                pltpu.make_async_copy(
                    ref.at[pl.ds(first, where.size)], t_buf.at[slot, where], t_sem.at[slot, k]
                )
                for k, (ref, (_, first), where) in enumerate(
                    zip(parts[n * j : n * j + n], tokens[j], at)
                )
            ]

        start_weight(meets(LATE[0], zn, yn)[1], 0, True)
        found, side = jnp.int32(0), [jnp.int32(0)] * 2
        for j, d in enumerate(FIRST + SECOND + THIRD):
            across, index = meets(d, zn, yn)
            for slot in range(2):
                here = jnp.logical_and(across == yn // 2, found == slot)
                side[slot] = jnp.where(here, index, side[slot])

                @pl.when(here)
                def _():
                    for copy in token_copies(late + j, slot):
                        copy.start()
            found = found + jnp.where(across == yn // 2, 1, 0)

        for j in range(late):
            slot = j % 2
            if j + 1 < late:
                start_weight(meets(LATE[j + 1], zn, yn)[1], 1 - slot, True)
            else:
                start_weight(side[0], 1 - slot, found > 0)
            weight_copy(0, slot).wait()
            for ref, (_, first), where, source in zip(
                parts[n * j : n * j + n], tokens[j], at, from_total
            ):
                before = total_ref[half, source, :] if j == 0 else out_ref[where, :]
                out_ref[where, :] = before + jnp.dot(
                    ref[first : first + where.size, :],
                    w_buf[slot],
                    preferred_element_type=jnp.float32,
                )

        def rest(k, carry):
            slot = lax.rem(late + k, 2)

            @pl.when(jnp.logical_and(k == 0, found > 1))
            def _():
                start_weight(side[1], 1 - late % 2, True)

            weight_copy(0, slot).wait()
            for copy in token_copies(late, k):
                copy.wait()

            def rows_of(i, carry):
                where = pl.ds(pl.multiple_of(i * (rows // 2), rows // 2), rows // 2)
                out_ref[where, :] += jnp.dot(
                    t_buf[k, where, :], w_buf[slot], preferred_element_type=jnp.float32
                )
                return carry

            return lax.fori_loop(0, wanted_rows // (rows // 2), rows_of, carry)

        lax.fori_loop(0, found, rest, 0)

    scratch = [
        pltpu.VMEM((2, wanted_rows, depth), jnp.bfloat16),
        pltpu.SemaphoreType.DMA((2, n)),
    ]
    arrays = [w for w, _ in weights]
    shape = (wanted_rows, width)
    return call(kernel, shape, 3, tokens, arrays, [total], scratch, {})


def finish(own, lower, upper):
    rows, width = own.shape
    chunk = rows // 4

    def kernel(own_ref, lower_ref, upper_ref, out_ref, buf, sem):
        def store(i):
            return pltpu.make_async_copy(
                buf.at[i], out_ref.at[pl.ds(i * chunk, chunk)], sem.at[i]
            )

        for i in range(4):
            source = lower_ref if i < 2 else upper_ref
            first = (i % 2) * chunk
            buf[i] = (
                own_ref[i * chunk : (i + 1) * chunk, :] + source[first : first + chunk, :]
            ).astype(jnp.bfloat16)
            if i:
                store(i - 1).start()
        store(3).start()
        for i in range(4):
            store(i).wait()

    return pl.pallas_call(
        kernel,
        name="finish",
        out_shape=jax.ShapeDtypeStruct((rows, width), jnp.bfloat16),
        in_specs=[VMEM] * 3,
        out_specs=ANYWHERE,
        scratch_shapes=[pltpu.VMEM((4, chunk, width), jnp.bfloat16), pltpu.SemaphoreType.DMA((4,))],
        compiler_params=pltpu.CompilerParams(vmem_limit_bytes=4 * 1024 * 1024),
        cost_estimate=pl.CostEstimate(
            flops=rows * width, bytes_accessed=10 * rows * width, transcendentals=0
        ),
    )(own, lower, upper)


def per_device(tokens, up_weight):
    _, _, _, core, xh = (lax.axis_index(axis) for axis in AXES)
    zn, yn = lax.axis_size("z"), lax.axis_size("y")
    rows, depth = tokens.shape
    nb = rows // 4
    width = up_weight.shape[1] // 2

    def up(axis, a):
        return lax.ppermute(a, axis, ring(lax.axis_size(axis), 1))

    def down(axis, a):
        return lax.ppermute(a, axis, ring(lax.axis_size(axis), -1))

    def crossed(a, shift):
        pairs = [
            (2 * i + k, 2 * ((i + shift) % yn) + 1 - k) for i in range(yn) for k in range(2)
        ]
        return lax.ppermute(a, ("y", "core"), pairs)

    def quarter(parity, layer):
        return lax.dynamic_slice(
            up_weight, (parity * depth, layer * width), (depth, width)
        )

    b, c, a = {}, {}, {}
    b[0] = lax.dynamic_slice_in_dim(tokens, xh * nb, nb, 0)
    c[0] = lax.dynamic_slice_in_dim(tokens, (1 - xh) * nb, nb, 0)
    a[0] = tokens[2 * nb :]
    mine, given, far = quarter(core, xh), quarter(1 - core, xh), quarter(1 - core, 1 - xh)

    b[-1], b[1] = up("z", b[0]), down("z", b[0])
    a[-1], a[1] = up("z", a[0]), down("z", a[0])
    b[-2], b[2] = up("z", b[-1]), down("z", b[1])
    a[-2], a[2] = up("z", a[-1]), down("z", a[1])
    b[-3], b[3] = up("z", b[-2]), down("z", b[2])
    a[-3], a[3] = up("z", a[-2]), down("z", a[2])
    b[4], a[4] = down("z", b[3]), up("z", a[-3])
    for d in (1, 2, 3):
        pair = lax.ppermute(jnp.concatenate([b[-d], b[d]], 0), "xh", ring(2, 1))
        c[-d], c[d] = (pair, 0), (pair, nb)
    c[0], c[4] = (c[0], 0), (lax.ppermute(b[4], "xh", ring(2, 1)), 0)

    wa, wb, wo = {0: mine}, {}, {}
    wa[-1], wa[1] = up("y", mine), down("y", mine)
    wb[-1], wb[1] = crossed(given, 1), crossed(given, -1)
    near = lax.ppermute(mine, "xl", ring(2, 1))
    across = lax.ppermute(far, ("xl", "core", "xh"), [(i, 7 - i) for i in range(8)])
    wb[0] = lax.ppermute(given, "core", ring(2, 1))
    wo[0] = jnp.concatenate([near, across], 1)
    wo[-1], wo[1] = up("y", wo[0]), down("y", wo[0])
    wide = jnp.concatenate([wa[-1], wb[-1]], 1)
    wide = up("y", wide)
    wo[2] = down("y", wo[1])

    def block(d):
        return [(a[d], 0), (b[d], 0), c[d]]

    first, second, third, late = (
        [block(d) for d in order] for order in (FIRST, SECOND, THIRD, LATE)
    )

    def weights(half, distances):
        listed = []
        for dy in distances:
            own = (wide, half * width) if dy == 2 else ((wb if half else wa)[dy], 0)
            listed += [own, (wo[dy], half * width)]
        return listed

    sizes = (rows, nb, zn, yn)
    near_weights = [weights(half, (0, 1, -1)) for half in range(2)]
    total = early_product(FIRST, None, first, near_weights, *sizes)
    total = early_product(SECOND, total, second, near_weights, *sizes)
    total = early_product(THIRD, total, third, near_weights, *sizes)

    def final(half, used):
        others = first + second + third
        far_weights = weights(half, (0, 1, 2, -1))
        return final_product(half, used, total, late, others, far_weights, *sizes)

    upper = lax.ppermute(final(1, (0,)), "core", ring(2, 1))
    lower = lax.ppermute(final(1, (1, 2)), "core", ring(2, 1))
    own = final(0, (0, 1, 2))
    return finish(own, lower, upper)


def solution(mesh):
    split = Mesh(
        mesh.devices.reshape(4, 2, mesh.shape["col"] // 2, 2, mesh.shape["layer"]), AXES
    )
    spec = P(("y", "xl"), ("z", "core"))
    return jax.shard_map(
        per_device,
        mesh=split,
        in_specs=(spec, spec),
        out_specs=P(("y", "xl"), ("z", "core", "xh")),
        check_vma=False,
    )
```

```python
import jax
import jax.numpy as jnp
from jax import lax
from jax.experimental import pallas as pl
from jax.experimental.pallas import tpu as pltpu
from jax.sharding import Mesh
from jax.sharding import PartitionSpec as P


AXES = ("y", "xl", "z", "core", "xh")
FIRST = (0, 1, -1)
SECOND = (2, -2)
THIRD = (3, -3)
EARLIER = FIRST + SECOND
LATE = (4,)


def ring(size, shift):
    return [(i, (i + shift) % size) for i in range(size)]


VMEM = pl.BlockSpec(memory_space=pltpu.VMEM)
ANYWHERE = pl.BlockSpec(memory_space=pl.ANY)


def meets(d, zn, yn):
    y, xl, z = (lax.axis_index(axis) for axis in ("y", "xl", "z"))
    block = lax.rem(z + d + zn, zn)
    across = lax.rem(block // 2 - y + yn, yn)
    return across, 2 * across + jnp.where(lax.rem(block, 2) == xl, 0, 1)


def places(rows, nb):
    xh = lax.axis_index("xh")
    return (
        pl.ds(2 * nb, rows - 2 * nb),
        pl.ds(pl.multiple_of(xh * nb, nb), nb),
        pl.ds(pl.multiple_of((1 - xh) * nb, nb), nb),
    )


def call(kernel, out_shape, blocks, tokens, weights, extra, scratch, aliases, far=()):
    rows, width = out_shape[-2:]
    depth = weights[0].shape[0]
    parts = [part for block in tokens for part, _ in block]
    return pl.pallas_call(
        kernel,
        out_shape=[jax.ShapeDtypeStruct(out_shape, jnp.float32)]
        + [jax.ShapeDtypeStruct(shape, jnp.bfloat16) for shape in far],
        in_specs=[VMEM] * (len(extra) + len(parts)) + [ANYWHERE] * len(weights),
        out_specs=[VMEM] * (1 + len(far)),
        input_output_aliases=aliases,
        scratch_shapes=[pltpu.VMEM((2, depth, width), jnp.bfloat16), pltpu.SemaphoreType.DMA((2,))]
        + scratch,
        compiler_params=pltpu.CompilerParams(vmem_limit_bytes=8 * 1024 * 1024),
        cost_estimate=pl.CostEstimate(
            flops=2 * rows * width * depth * blocks,
            bytes_accessed=2 * blocks * depth * (rows + width) + 4 * rows * width,
            transcendentals=0,
        ),
    )(*extra, *parts, *weights)


def early_product(order, total, tokens, near_weights, rows, nb, zn, yn, others=None):
    width = near_weights[0][0][0].shape[1]
    arrays = [w for half in near_weights for w, _ in half]
    known = (0, 1, 2, 3, 2 * yn - 2, 2 * yn - 1)
    totals = [] if total is None else [total]
    blocks = tokens + ([] if others is None else others)

    def kernel(*refs):
        tail = 3 if others is None else 5
        refs, tail = refs[len(totals) : -tail], refs[-tail:]
        if others is None:
            out_ref, w_buf, sem = tail
        else:
            out_ref, far_ref, w_buf, sem, far_sem = tail
        parts, w_refs = refs[: 3 * len(blocks)], refs[3 * len(blocks) :]
        at = places(rows, nb)

        def pick(j, slot):
            return [
                pltpu.make_async_copy(
                    ref.at[pl.ds(first, where.size)],
                    far_ref.at[slot, where],
                    far_sem.at[slot, k],
                )
                for k, (ref, (_, first), where) in enumerate(
                    zip(parts[3 * j : 3 * j + 3], blocks[j], at)
                )
            ]

        found = jnp.int32(0)
        if others is not None:
            for d in EARLIER + order:
                j = order.index(d) if d in order else len(order) + EARLIER.index(d)
                far_off = meets(d, zn, yn)[0] == yn // 2
                for slot in range(2):
                    @pl.when(jnp.logical_and(far_off, found == slot))
                    def _():
                        for one in pick(j, slot):
                            one.start()
                found = found + jnp.where(far_off, 1, 0)

        def copy(half, i, slot):
            return pltpu.make_async_copy(
                w_refs[6 * half + i].at[:, pl.ds(near_weights[half][i][1], width)],
                w_buf.at[slot],
                sem.at[slot],
            )

        def start(turn, d, slot):
            _, index = meets(d, zn, yn)
            for half in range(2):
                for i, number in enumerate(known):
                    @pl.when(jnp.logical_and(turn == half, index == number))
                    def _():
                        copy(half, i, slot).start()

        def both(turn, carry):
            if total is None:
                out_ref[turn] = jnp.zeros((rows, width), jnp.float32)
            start(turn, order[0], 0)
            for j, d in enumerate(order):
                slot = j % 2
                if j + 1 < len(order):
                    start(turn, order[j + 1], 1 - slot)

                @pl.when(meets(d, zn, yn)[0] != yn // 2)
                def _():
                    copy(0, 0, slot).wait()
                    for ref, (part, first), where in zip(parts[3 * j : 3 * j + 3], tokens[j], at):
                        out_ref[turn, where, :] += jnp.dot(
                            ref[first : first + where.size, :],
                            w_buf[slot],
                            preferred_element_type=jnp.float32,
                        )

            return carry

        lax.fori_loop(0, 2, both, 0)
        if others is not None:
            for slot in range(2):
                @pl.when(found > slot)
                def _():
                    for one in pick(0, slot):
                        one.wait()

    aliases = {i: 0 for i in range(len(totals))}
    pairs, shape, depth = 2 * len(order), (2, rows, width), near_weights[0][0][0].shape[0]
    if others is None:
        return call(kernel, shape, pairs, blocks, arrays, totals, [], aliases)[0]
    far, sems = [(2, rows, depth)], [pltpu.SemaphoreType.DMA((2, 3))]
    return call(kernel, shape, pairs, blocks, arrays, totals, sems, aliases, far)


def final_product(half, used, total, far, late_tokens, weights, rows, nb, zn, yn):
    width = total.shape[2]
    tokens = [[block[part] for part in used] for block in late_tokens]
    late, n = len(LATE), len(used)
    base = 2 * nb if used == (0,) else 0
    wanted_rows = sum((rows - 2 * nb, nb, nb)[part] for part in used)

    def kernel(total_ref, far_ref, *refs):
        parts, w_refs = refs[: n * len(tokens)], refs[n * len(tokens) : -3]
        out_ref, w_buf, w_sem = refs[-3:]
        from_total = [places(rows, nb)[part] for part in used]
        at = [pl.ds(0, where.size) if base else where for where in from_total]

        def weight_copy(i, slot):
            return pltpu.make_async_copy(
                w_refs[i].at[:, pl.ds(weights[i][1], width)], w_buf.at[slot], w_sem.at[slot]
            )

        def start_weight(index, slot, wanted):
            for i in range(len(weights)):
                @pl.when(jnp.logical_and(wanted, index == i))
                def _():
                    weight_copy(i, slot).start()

        start_weight(meets(LATE[0], zn, yn)[1], 0, True)
        found, side = jnp.int32(0), [jnp.int32(0)] * 2
        for d in EARLIER + THIRD:
            across, index = meets(d, zn, yn)
            for slot in range(2):
                here = jnp.logical_and(across == yn // 2, found == slot)
                side[slot] = jnp.where(here, index, side[slot])
            found = found + jnp.where(across == yn // 2, 1, 0)

        for j in range(late):
            slot = j % 2
            if j + 1 < late:
                start_weight(meets(LATE[j + 1], zn, yn)[1], 1 - slot, True)
            else:
                start_weight(side[0], 1 - slot, found > 0)
            weight_copy(0, slot).wait()
            for ref, (_, first), where, source in zip(
                parts[n * j : n * j + n], tokens[j], at, from_total
            ):
                before = total_ref[half, source, :] if j == 0 else out_ref[where, :]
                out_ref[where, :] = before + jnp.dot(
                    ref[first : first + where.size, :],
                    w_buf[slot],
                    preferred_element_type=jnp.float32,
                )

        def rest(k, carry):
            slot = lax.rem(late + k, 2)

            @pl.when(jnp.logical_and(k == 0, found > 1))
            def _():
                start_weight(side[1], 1 - late % 2, True)

            weight_copy(0, slot).wait()

            def rows_of(i, carry):
                where = pl.ds(pl.multiple_of(i * (rows // 2), rows // 2), rows // 2)
                source = pl.ds(pl.multiple_of(base + i * (rows // 2), rows // 2), rows // 2)
                out_ref[where, :] += jnp.dot(
                    far_ref[k, source, :], w_buf[slot], preferred_element_type=jnp.float32
                )
                return carry

            return lax.fori_loop(0, wanted_rows // (rows // 2), rows_of, carry)

        lax.fori_loop(0, found, rest, 0)

    arrays = [w for w, _ in weights]
    shape = (wanted_rows, width)
    return call(kernel, shape, 3, tokens, arrays, [total, far], [], {})[0]


def finish(own, lower, upper):
    rows, width = own.shape
    chunk = rows // 4

    def kernel(own_ref, lower_ref, upper_ref, out_ref, buf, sem):
        def store(i):
            return pltpu.make_async_copy(
                buf.at[i], out_ref.at[pl.ds(i * chunk, chunk)], sem.at[i]
            )

        for i in range(4):
            source = lower_ref if i < 2 else upper_ref
            first = (i % 2) * chunk
            buf[i] = (
                own_ref[i * chunk : (i + 1) * chunk, :] + source[first : first + chunk, :]
            ).astype(jnp.bfloat16)
            if i:
                store(i - 1).start()
        store(3).start()
        for i in range(4):
            store(i).wait()

    return pl.pallas_call(
        kernel,
        name="finish",
        out_shape=jax.ShapeDtypeStruct((rows, width), jnp.bfloat16),
        in_specs=[VMEM] * 3,
        out_specs=ANYWHERE,
        scratch_shapes=[pltpu.VMEM((4, chunk, width), jnp.bfloat16), pltpu.SemaphoreType.DMA((4,))],
        compiler_params=pltpu.CompilerParams(vmem_limit_bytes=4 * 1024 * 1024),
        cost_estimate=pl.CostEstimate(
            flops=rows * width, bytes_accessed=10 * rows * width, transcendentals=0
        ),
    )(own, lower, upper)


def per_device(tokens, up_weight):
    _, _, _, core, xh = (lax.axis_index(axis) for axis in AXES)
    zn, yn = lax.axis_size("z"), lax.axis_size("y")
    rows, depth = tokens.shape
    nb = rows // 4
    width = up_weight.shape[1] // 2

    def up(axis, a):
        return lax.ppermute(a, axis, ring(lax.axis_size(axis), 1))

    def down(axis, a):
        return lax.ppermute(a, axis, ring(lax.axis_size(axis), -1))

    def crossed(a, shift):
        pairs = [
            (2 * i + k, 2 * ((i + shift) % yn) + 1 - k) for i in range(yn) for k in range(2)
        ]
        return lax.ppermute(a, ("y", "core"), pairs)

    def quarter(parity, layer):
        return lax.dynamic_slice(
            up_weight, (parity * depth, layer * width), (depth, width)
        )

    b, c, a = {}, {}, {}
    b[0] = lax.dynamic_slice_in_dim(tokens, xh * nb, nb, 0)
    c[0] = lax.dynamic_slice_in_dim(tokens, (1 - xh) * nb, nb, 0)
    a[0] = tokens[2 * nb :]
    mine, given, away = quarter(core, xh), quarter(1 - core, xh), quarter(1 - core, 1 - xh)

    b[-1], b[1] = up("z", b[0]), down("z", b[0])
    a[-1], a[1] = up("z", a[0]), down("z", a[0])
    b[-2], b[2] = up("z", b[-1]), down("z", b[1])
    a[-2], a[2] = up("z", a[-1]), down("z", a[1])
    b[-3], b[3] = up("z", b[-2]), down("z", b[2])
    a[-3], a[3] = up("z", a[-2]), down("z", a[2])
    b[4], a[4] = down("z", b[3]), up("z", a[-3])
    for d in (1, 2, 3):
        pair = lax.ppermute(jnp.concatenate([b[-d], b[d]], 0), "xh", ring(2, 1))
        c[-d], c[d] = (pair, 0), (pair, nb)
    c[0], c[4] = (c[0], 0), (lax.ppermute(b[4], "xh", ring(2, 1)), 0)

    wa, wb, wo = {0: mine}, {}, {}
    wa[-1], wa[1] = up("y", mine), down("y", mine)
    wb[-1], wb[1] = crossed(given, 1), crossed(given, -1)
    near = lax.ppermute(mine, "xl", ring(2, 1))
    across = lax.ppermute(away, ("xl", "core", "xh"), [(i, 7 - i) for i in range(8)])
    wb[0] = lax.ppermute(given, "core", ring(2, 1))
    wo[0] = jnp.concatenate([near, across], 1)
    wo[-1], wo[1] = up("y", wo[0]), down("y", wo[0])
    wide = jnp.concatenate([wa[-1], wb[-1]], 1)
    wide = up("y", wide)
    wo[2] = down("y", wo[1])

    def block(d):
        return [(a[d], 0), (b[d], 0), c[d]]

    first, second, third, late = (
        [block(d) for d in order] for order in (FIRST, SECOND, THIRD, LATE)
    )

    def weights(half, distances):
        listed = []
        for dy in distances:
            own = (wide, half * width) if dy == 2 else ((wb if half else wa)[dy], 0)
            listed += [own, (wo[dy], half * width)]
        return listed

    sizes = (rows, nb, zn, yn)
    near_weights = [weights(half, (0, 1, -1)) for half in range(2)]
    total = early_product(FIRST, None, first, near_weights, *sizes)
    total = early_product(SECOND, total, second, near_weights, *sizes)
    total, far = early_product(THIRD, total, third, near_weights, *sizes, first + second)

    def final(half, used):
        all_weights = weights(half, (0, 1, 2, -1))
        return final_product(half, used, total, far, late, all_weights, *sizes)

    upper = lax.ppermute(final(1, (0,)), "core", ring(2, 1))
    lower = lax.ppermute(final(1, (1, 2)), "core", ring(2, 1))
    own = final(0, (0, 1, 2))
    return finish(own, lower, upper)


def solution(mesh):
    split = Mesh(
        mesh.devices.reshape(4, 2, mesh.shape["col"] // 2, 2, mesh.shape["layer"]), AXES
    )
    spec = P(("y", "xl"), ("z", "core"))
    return jax.shard_map(
        per_device,
        mesh=split,
        in_specs=(spec, spec),
        out_specs=P(("y", "xl"), ("z", "core", "xh")),
        check_vma=False,
    )
```
